32 devices in a mesh: dp: 4 (over z), tp: 8 (over y, x, core).
Axes of the slice: x: 2, y: 2, z: 4, core: 2. Of those that a mesh axis runs over, the one named last changes fastest.
Arguments:
- layer_input: bfloat16 [8192, 2048], P(('dp', 'tp')), may hold values from -6 to 6
- segments: int32 [4, 2048], P('dp'), may hold values from 0 to 1, as said below
- norm_gains: float32 [2, 2048], replicated, may hold values from 0.25 to 1.75
- norm_biases: float32 [2, 2048], replicated, may hold values from -2 to 2
- w_qkv: bfloat16 [2048, 3, 2048], P(None, None, 'tp'), may hold values from -0.125 to 0.125
- qv_bias: float32 [2, 2048], P(None, 'tp'), may hold values from -2 to 2
- key_bias: float32 [32, 16], P('tp'), may hold values from -3 to 3
- w_out: bfloat16 [2048, 2048], P('tp'), may hold values from -2 to 2
- w_gate_up: bfloat16 [2048, 2, 5632], P(None, None, 'tp'), may hold values from -0.125 to 0.125
- w_down: bfloat16 [5632, 2048], P('tp'), may hold values from -0.078125 to 0.078125
- out_grad: bfloat16 [8192, 2048], P(('dp', 'tp')), may hold values from -6 to 6
Outputs:
- output: float32 [8192, 2048], P(('dp', 'tp'))
- grad_x: float32 [8192, 2048], P(('dp', 'tp'))
- grad_qkv: float32 [2048, 3, 2048], P(None, None, 'tp')
- grad_qv_bias: float32 [2, 2048], P(None, 'tp')
- grad_key_bias: float32 [32, 16], P('tp')
- grad_out: float32 [2048, 2048], P('tp')
- grad_gate_up: float32 [2048, 2, 5632], P(None, None, 'tp')
- grad_down: float32 [5632, 2048], P('tp')
- grad_gains: float32 [2, 2048], P(None, 'tp')
- grad_biases: float32 [2, 2048], P(None, 'tp')
The draws below stay inside these ranges and needn't reach their ends.
Inputs may be any that keep to these rules, and one draw needn't show every extreme that they name: `segments`: in each group the ids number the documents from 0 and never fall; every document has 1024 tokens or more.
All inputs are finite; a program needn't handle non-finite values.
Results may differ from the reference program's by a relative error of at most 0.023.
Values may be sent and summed in bfloat16 or wider, within the bound.
A program may use at most 256 MiB of HBM per device.

```python
import math
import jax
import jax.numpy as jnp
from jax import lax

D = 2048
HEADS = 32
HEAD_DIM = 64
FF = 5632
ROT = 16
MIN_DOC = 1024
GROUP = 2048
TOKENS = 8192
N_DP = 4
N_TP = 8


def draw_segments(key, part):
    most = GROUP // MIN_DOC
    slots = max(most - 1, 1)
    key_count = jax.random.fold_in(key, 11)
    key_full = jax.random.fold_in(key, 12)
    key_cuts = jax.random.fold_in(key, 13)
    counts = jax.random.randint(key_count, (N_DP,), 1, most + 1)
    full_group = jax.random.randint(key_full, (), 0, N_DP)
    counts = jnp.where(jnp.arange(N_DP) == full_group, most, counts)
    slack = GROUP - counts * MIN_DOC
    cuts = jax.random.randint(key_cuts, (N_DP, slots), 0, slack[:, None] + 1)
    slot_index = jnp.arange(slots)[None, :]
    used = slot_index < counts[:, None] - 1
    cuts = jnp.sort(jnp.where(used, cuts, slack[:, None]), axis=1)
    starts = jnp.where(used, (slot_index + 1) * MIN_DOC + cuts, GROUP)
    places = jnp.arange(GROUP)
    return jnp.sum((places[None, :, None] >= starts[:, None, :]).astype(jnp.int32), axis=2).astype(jnp.int32)


def shard_levels(own_key, extent, cuts, low, top_value):
    loudness = 1.0
    for axis_at, blocks in cuts:
        draws = jax.random.uniform(jax.random.fold_in(jax.random.fold_in(own_key, 6), axis_at), (blocks,), jnp.float32, low / len(cuts), top_value / len(cuts))
        loudness = loudness * jnp.repeat(jnp.exp(draws), extent[axis_at] // blocks).reshape((-1,) + (1,) * (len(extent) - 1 - axis_at))
    return loudness


def gaussian(stream_key, dims, scale, limit, cuts=(), kind=jnp.bfloat16):
    result = scale * jax.random.normal(stream_key, dims, jnp.float32)
    if cuts:
        result = result * shard_levels(stream_key, dims, cuts, -0.22, 0.18)
    return jnp.clip(result, -limit, limit).astype(kind)


def setup_inputs(seed: int = 0) -> dict:
    seeds = jax.random.split(jax.random.key(seed), 12)
    layer_input = gaussian(seeds[0], (TOKENS, D), 1.0, 6.0, ((0, 32),))
    segments = draw_segments(jax.random.fold_in(seeds[11], 71), 0)
    norm_gains = jnp.clip(1.0 + 0.15 * jax.random.normal(seeds[2], (2, D), jnp.float32), 0.25, 1.75)
    norm_biases = gaussian(seeds[3], (2, D), 0.3, 2.0, (), jnp.float32)
    w_qkv = gaussian(seeds[4], (D, 3, D), D ** -0.5, 0.125, ((2, 8),))
    qv_bias = gaussian(seeds[5], (2, D), 0.3, 2.0, ((1, 8),), jnp.float32)
    key_bias = gaussian(seeds[6], (HEADS, ROT), 0.5, 3.0, ((0, 8),), jnp.float32)
    w_out = gaussian(seeds[7], (D, D), (max(D // 256, 1)) ** -0.5, 2.0, ((0, 8),))
    w_gate_up = gaussian(seeds[8], (D, 2, FF), D ** -0.5, 0.125, ((2, 8),))
    w_down = gaussian(seeds[9], (FF, D), FF ** -0.5, 0.078125, ((0, 8),))
    out_grad = gaussian(seeds[10], (TOKENS, D), 1.0, 6.0, ((0, 32),))
    return dict(layer_input=layer_input, segments=segments, norm_gains=norm_gains, norm_biases=norm_biases, w_qkv=w_qkv, qv_bias=qv_bias, key_bias=key_bias, w_out=w_out, w_gate_up=w_gate_up, w_down=w_down, out_grad=out_grad)


@jax.custom_vjp
def low(v):
    return lax.optimization_barrier(v.astype(jnp.bfloat16)).astype(jnp.float32)

@jax.custom_vjp
def low_back(v):
    return v

def low_keep(v):
    return (low(v), None)

def low_pass(kept, grad):
    return (grad,)

def back_keep(v):
    return (v, None)

def back_low(kept, grad):
    return (low(grad),)
low.defvjp(low_keep, low_pass)
low_back.defvjp(back_keep, back_low)

def product(left, right):
    return jnp.dot(left, right, precision=lax.Precision.HIGHEST)

def layer_norm(values, gain, shift_bias):
    centre = lax.optimization_barrier(jnp.mean(values, axis=-1, keepdims=True))
    centred = values - centre
    spread = lax.optimization_barrier(jnp.mean(centred * centred, axis=-1, keepdims=True))
    return centred * lax.rsqrt(spread + 1e-05) * gain + shift_bias

def rotary_tables(segment_ids):
    places = jnp.arange(segment_ids.shape[0], dtype=jnp.int32)
    starts_here = jnp.concatenate([jnp.ones((1,), dtype=jnp.bool_), segment_ids[1:] != segment_ids[:-1]])
    doc_start = lax.cummax(jnp.where(starts_here, places, 0), axis=0)
    positions = (places - doc_start).astype(jnp.float32)
    halves = ROT // 2
    frequency = jnp.exp(jnp.arange(halves, dtype=jnp.float32) * (-2.0 * math.log(10000.0) / ROT))
    angles = positions[:, None] * frequency[None, :]
    return (jnp.cos(angles)[:, None, :], jnp.sin(angles)[:, None, :])

def rotate(tensor, cosine, sine):
    halves = ROT // 2
    first_half = tensor[..., :halves]
    second_half = tensor[..., halves:ROT]
    return jnp.concatenate([first_half * cosine - second_half * sine, second_half * cosine + first_half * sine, tensor[..., ROT:]], axis=-1)

def head_attention(queries, keys_head, values_head, visible):
    scores = low_back(product(queries, keys_head.T) * HEAD_DIM ** (-0.5))
    weights = jax.nn.softmax(jnp.where(visible, scores, -jnp.inf), axis=-1)
    return product(low(weights), values_head)

def sharded_columns(normed, weight, parts, rows):
    width = weight.shape[2] // N_TP
    split = weight.reshape(D, parts, N_TP, width)
    pieces = []
    for shard in range(N_TP):
        pieces.append(product(low_back(normed), split[:, :, shard].reshape(D, parts * width)).reshape(rows, parts, width))
    return jnp.stack(pieces, axis=2).reshape(rows, parts, N_TP * width)

def sharded_rows(left, weight):
    width = left.shape[1] // N_TP
    total = jnp.zeros((left.shape[0], weight.shape[1]), jnp.float32)
    for shard in range(N_TP):
        total = total + low(product(left[:, shard * width:(shard + 1) * width], weight[shard * width:(shard + 1) * width]))
    return total

def group_layer(group_x, segment_ids, norm_gains, norm_biases, w_qkv, qv_bias, key_bias, w_out, w_gate_up, w_down):
    rows = group_x.shape[0]
    cosine, sine = rotary_tables(segment_ids)
    places = jnp.arange(rows, dtype=jnp.int32)
    visible = (segment_ids[:, None] == segment_ids[None, :]) & (places[:, None] >= places[None, :])
    normed_one = low(layer_norm(group_x, norm_gains[0], norm_biases[0]))
    projected = sharded_columns(normed_one, w_qkv, 3, rows).reshape(rows, 3, HEADS, HEAD_DIM)
    key_full = jnp.concatenate([key_bias, jnp.zeros((HEADS, HEAD_DIM - ROT), jnp.float32)], axis=1)
    bias_all = jnp.stack([qv_bias[0].reshape(HEADS, HEAD_DIM), key_full, qv_bias[1].reshape(HEADS, HEAD_DIM)])
    projected = low_back(projected + bias_all[None])
    queries = low(rotate(projected[:, 0], cosine, sine))
    key_rows = low(rotate(projected[:, 1], cosine, sine))
    value_rows = low(projected[:, 2])

    def one_head(item):
        return jax.checkpoint(head_attention)(item[0], item[1], item[2], visible)
    heads_out = lax.map(one_head, (queries.transpose(1, 0, 2), key_rows.transpose(1, 0, 2), value_rows.transpose(1, 0, 2)))
    attended = low(low_back(heads_out.transpose(1, 0, 2).reshape(rows, D)))
    hidden = group_x + low_back(sharded_rows(attended, w_out))
    normed_two = low(layer_norm(hidden, norm_gains[1], norm_biases[1]))
    gate_up = low_back(sharded_columns(normed_two, w_gate_up, 2, rows))
    activation = low(jax.nn.silu(gate_up[:, 0]) * gate_up[:, 1])
    return hidden + low_back(sharded_rows(activation, w_down))

def reference(layer_input, segments, norm_gains, norm_biases, w_qkv, qv_bias, key_bias, w_out, w_gate_up, w_down, out_grad):
    params = (norm_gains, norm_biases, w_qkv.astype(jnp.float32), qv_bias, key_bias, w_out.astype(jnp.float32), w_gate_up.astype(jnp.float32), w_down.astype(jnp.float32))

    def forward(x_float, weights):
        groups = x_float.reshape(N_DP, GROUP, D)

        def one_group(item):
            return group_layer(item[0], item[1], *weights)
        return lax.map(jax.checkpoint(one_group), (groups, segments)).reshape(N_DP * GROUP, D)
    output, pullback = jax.vjp(forward, layer_input.astype(jnp.float32), params)
    grad_x, grads = pullback(out_grad.astype(jnp.float32))
    return (output, grad_x, grads[2], grads[3], grads[4], grads[5], grads[6], grads[7], grads[0], grads[1])
```

```python
import functools
import math

import jax
import jax.numpy as jnp
from jax import lax
from jax.experimental import pallas as pl
from jax.experimental.pallas import tpu as pltpu
from jax.sharding import PartitionSpec as P

D = 2048
HEAD_DIM = 64
ROT = 16
EPSILON = 1e-05
MESH = pl.DeviceIdType.MESH
NT = (((1,), (1,)), ((), ()))
TN = (((0,), (0,)), ((), ()))


def norm_forward(values, gain, shift_bias):
    centre = jnp.mean(values, axis=-1, keepdims=True)
    centred = values - centre
    spread = jnp.mean(centred * centred, axis=-1, keepdims=True)
    inverse = lax.rsqrt(spread + EPSILON)
    normed = centred * inverse
    return (normed * gain + shift_bias, normed, inverse)


def norm_backward(grad_normed, normed, inverse, gain):
    scaled = grad_normed * gain
    inner = jnp.mean(scaled, axis=-1, keepdims=True)
    along = jnp.mean(scaled * normed, axis=-1, keepdims=True)
    return (
        inverse * (scaled - inner - normed * along),
        jnp.sum(grad_normed * normed, axis=0),
        jnp.sum(grad_normed, axis=0),
    )


def contract_rows(left, right):
    return lax.dot_general(left, right, TN, preferred_element_type=jnp.float32)


def contract_cols(left, right):
    return lax.dot_general(left, right, NT, preferred_element_type=jnp.float32)


def whole(shape):
    return pl.BlockSpec(shape, lambda step: (0,) * len(shape))


def turn(values, table, flip, lane):
    width = values.shape[1]
    ahead = pltpu.roll(values, width - ROT // 2, 1)
    behind = pltpu.roll(values, ROT // 2, 1)
    return values * table + jnp.where(lane < ROT // 2, ahead, behind) * flip


def rotary_tables(segment_ids):
    places = jnp.arange(segment_ids.shape[0], dtype=jnp.int32)
    fresh = jnp.concatenate([jnp.ones((1,), jnp.bool_), segment_ids[1:] != segment_ids[:-1]])
    starts = lax.cummax(jnp.where(fresh, places, 0), axis=0)
    halves = ROT // 2
    lane = jnp.arange(128, dtype=jnp.int32) % HEAD_DIM
    frequency = jnp.exp((lane % halves).astype(jnp.float32) * (-2.0 * math.log(10000.0) / ROT))
    frequency = jnp.where(lane < ROT, frequency, 0.0)
    angles = (places - starts).astype(jnp.float32)[:, None] * frequency[None, :]
    sign = jnp.where(lane < halves, -1.0, 1.0).astype(jnp.float32)
    return jnp.cos(angles), jnp.sin(angles) * sign[None, :], starts


def project_kernel(x_ref, w_ref, bias_ref, cos_ref, sin_ref, q_ref, k_ref, v_ref):
    width = q_ref.shape[1]
    value = jnp.dot(x_ref[...], w_ref[...], preferred_element_type=jnp.float32) + bias_ref[:1, :]
    lane = lax.broadcasted_iota(jnp.int32, (1, width), 1) % HEAD_DIM
    table = jnp.tile(cos_ref[...], (1, width // 128))
    flip = jnp.tile(sin_ref[...], (1, width // 128))
    q_ref[...] = turn(value[:, :width], table, flip, lane).astype(jnp.bfloat16)
    k_ref[...] = turn(value[:, width:2 * width], table, flip, lane).astype(jnp.bfloat16)
    v_ref[...] = value[:, 2 * width:].astype(jnp.bfloat16)


def project(x, w, bias, cos, sin):
    rows = x.shape[0]
    width = w.shape[1] // 3
    block = min(512, rows)
    tall = lambda cols: pl.BlockSpec((block, cols), lambda step: (step, 0))
    return pl.pallas_call(
        project_kernel,
        grid=(rows // block,),
        in_specs=[tall(D), whole(w.shape), whole(bias.shape), tall(128), tall(128)],
        out_specs=[tall(width)] * 3,
        out_shape=[jax.ShapeDtypeStruct((rows, width), jnp.bfloat16)] * 3,
        cost_estimate=pl.CostEstimate(flops=2 * rows * D * 3 * width, bytes_accessed=2 * rows * D + 12 * D * width, transcendentals=0),
        name="project",
    )(x, w, bias, cos, sin)


def forward_kernel(block, q_ref, k_ref, v_ref, start_ref, out_ref, lse_ref):
    head = pl.program_id(0)
    rows, width = q_ref.shape
    own = lax.broadcasted_iota(jnp.int32, (1, width), 1) // HEAD_DIM == head
    for index in range(rows // block):
        low, high = index * block, (index + 1) * block
        query = jnp.where(own, q_ref[low:high, :] * jnp.bfloat16(HEAD_DIM**-0.5), jnp.bfloat16(0))
        scores = lax.dot_general(query, k_ref[:high, :], NT, preferred_element_type=jnp.float32)
        key_place = lax.broadcasted_iota(jnp.int32, (block, high), 1)
        place = low + lax.broadcasted_iota(jnp.int32, (block, high), 0)
        seen = (key_place >= start_ref[low:high, :1]) & (key_place <= place)
        scores = jnp.where(seen, scores, -jnp.inf)
        top = jnp.max(scores, axis=1, keepdims=True)
        expo = jnp.exp(scores - top)
        total = jnp.sum(expo, axis=1, keepdims=True)
        mixed = jnp.dot(expo.astype(jnp.bfloat16), v_ref[:high, :], preferred_element_type=jnp.float32)
        mixed = (mixed / total).astype(jnp.bfloat16)

        @pl.when(head == 0)
        def _():
            out_ref[low:high, :] = mixed

        @pl.when(head > 0)
        def _():
            out_ref[low:high, :] = jnp.where(own, mixed, out_ref[low:high, :])

        spread = jnp.broadcast_to(top + jnp.log(total), (block, 128))
        lse_ref[0, :, low:high] = jnp.transpose(spread)[:8, :]


def attention_forward(q, k, v, start, block=256):
    rows, width = q.shape
    heads = width // HEAD_DIM
    return pl.pallas_call(
        functools.partial(forward_kernel, block),
        grid=(heads,),
        in_specs=[whole((rows, width))] * 3 + [whole((rows, 128))],
        out_specs=[whole((rows, width)), pl.BlockSpec((1, 8, rows), lambda step: (step, 0, 0))],
        out_shape=[
            jax.ShapeDtypeStruct((rows, width), jnp.bfloat16),
            jax.ShapeDtypeStruct((heads, 8, rows), jnp.float32),
        ],
        cost_estimate=pl.CostEstimate(flops=8 * rows * rows * width, bytes_accessed=12 * rows * width, transcendentals=rows * rows * heads // 2),
        name="attention_forward",
    )(q, k, v, start)


def backward_kernel(
    block, q_ref, k_ref, v_ref, o_ref, g_ref, lse_ref, start_ref, cos_ref, sin_ref, out_ref, sums_ref, dq, dk, dv, delta
):
    head = pl.program_id(0)
    rows, width = q_ref.shape
    heads = width // HEAD_DIM
    own = lax.broadcasted_iota(jnp.int32, (1, width), 1) // HEAD_DIM == head

    @pl.when(head == 0)
    def _():
        dq[...] = jnp.zeros_like(dq)
        dk[...] = jnp.zeros_like(dk)
        dv[...] = jnp.zeros_like(dv)

    pick = (own & (lax.broadcasted_iota(jnp.int32, (8, width), 0) >= 0)).astype(jnp.float32)
    product = g_ref[...].astype(jnp.float32) * o_ref[...].astype(jnp.float32)
    delta[...] = lax.dot_general(pick, product, NT, precision=lax.Precision.HIGHEST, preferred_element_type=jnp.float32)
    zero = jnp.bfloat16(0)
    for index in range(rows // block):
        low, high = index * block, (index + 1) * block
        span = rows - low
        key = jnp.where(own, k_ref[low:high, :], zero)
        value = jnp.where(own, v_ref[low:high, :], zero)
        query = q_ref[low:, :]
        grad = g_ref[low:, :]
        scores = lax.dot_general(key * jnp.bfloat16(HEAD_DIM**-0.5), query, NT, preferred_element_type=jnp.float32)
        key_place = low + lax.broadcasted_iota(jnp.int32, (block, span), 0)
        place = low + lax.broadcasted_iota(jnp.int32, (block, span), 1)
        seen = (key_place >= start_ref[:1, low:]) & (key_place <= place)
        weights = jnp.exp(jnp.where(seen, scores, -jnp.inf) - lse_ref[0, :1, low:])
        grad_probs = lax.dot_general(value, grad, NT, preferred_element_type=jnp.float32)
        grad_scores = (weights * (grad_probs - delta[:1, low:])).astype(jnp.bfloat16)
        probs = weights.astype(jnp.bfloat16)
        dv[low:high, :] += jnp.where(own, jnp.dot(probs, grad, preferred_element_type=jnp.float32), 0.0)
        dk[low:high, :] += jnp.where(own, jnp.dot(grad_scores, query, preferred_element_type=jnp.float32), 0.0)
        dq[low:, :] += lax.dot_general(grad_scores, key, TN, preferred_element_type=jnp.float32)

    @pl.when(head == heads - 1)
    def _():
        lane = lax.broadcasted_iota(jnp.int32, (1, width), 1) % HEAD_DIM
        step = min(256, rows)
        sums_ref[...] = jnp.zeros_like(sums_ref)

        @pl.loop(0, rows // step)
        def _(index):
            here = pl.ds(pl.multiple_of(index * step, step), step)
            table = jnp.tile(cos_ref[here, :], (1, width // 128))
            flip = -jnp.tile(sin_ref[here, :], (1, width // 128))
            for part, source in enumerate((dq, dk, dv)):
                value = source[here, :]
                if part < 2:
                    value = turn(value * HEAD_DIM**-0.5, table, flip, lane)
                value = value.astype(jnp.bfloat16)
                columns = slice(part * width, (part + 1) * width)
                out_ref[here, columns] = value
                total = jnp.sum(value.astype(jnp.float32), axis=0, keepdims=True)
                sums_ref[:, columns] += jnp.broadcast_to(total, (8, width))


def attention_backward(q, k, v, out, grad, lse, start, cos, sin, block=256):
    rows, width = q.shape
    heads = width // HEAD_DIM
    return pl.pallas_call(
        functools.partial(backward_kernel, block),
        grid=(heads,),
        in_specs=[whole((rows, width))] * 5
        + [pl.BlockSpec((1, 8, rows), lambda step: (step, 0, 0)), whole((8, rows)), whole((rows, 128)), whole((rows, 128))],
        out_specs=[whole((rows, 3 * width)), whole((8, 3 * width))],
        out_shape=[
            jax.ShapeDtypeStruct((rows, 3 * width), jnp.bfloat16),
            jax.ShapeDtypeStruct((8, 3 * width), jnp.float32),
        ],
        scratch_shapes=[pltpu.VMEM((rows, width), jnp.float32)] * 3 + [pltpu.VMEM((8, rows), jnp.float32)],
        cost_estimate=pl.CostEstimate(flops=20 * rows * rows * width, bytes_accessed=20 * rows * width, transcendentals=rows * rows * heads // 2),
        name="attention_backward",
    )(q, k, v, out, grad, lse, start, cos, sin)


def small_sums_kernel(
    n_tp, n_dp, norms_ref, heads_ref, out_ref, slots, total, planes, send_one, recv_one, send_two, recv_two
):
    tp, dp = lax.axis_index("tp"), lax.axis_index("dp")
    width = out_ref.shape[1]
    barrier = pltpu.get_barrier_semaphore()
    for hop in range(1, n_tp):
        pl.semaphore_signal(barrier, inc=1, device_id={"tp": lax.rem(tp + hop, n_tp)}, device_id_type=MESH)
    for hop in range(1, n_dp):
        pl.semaphore_signal(barrier, inc=1, device_id={"dp": lax.rem(dp + hop, n_dp)}, device_id_type=MESH)
    pl.semaphore_wait(barrier, n_tp + n_dp - 2)
    copies = []
    for hop in range(1, n_tp):
        peer = lax.rem(tp + hop, n_tp)
        copies.append(
            pltpu.make_async_remote_copy(
                src_ref=norms_ref.at[peer],
                dst_ref=slots.at[hop],
                send_sem=send_one.at[hop],
                recv_sem=recv_one.at[hop],
                device_id={"tp": peer},
                device_id_type=MESH,
            )
        )
    for copy in copies:
        copy.start()
    value = heads_ref[...] + norms_ref[tp]
    for copy in copies:
        copy.wait()
    for hop in range(1, n_tp):
        value = value + slots[hop]
    total[...] = value
    copies = []
    for hop in range(1, n_dp):
        copies.append(
            pltpu.make_async_remote_copy(
                src_ref=total,
                dst_ref=planes.at[dp],
                send_sem=send_two.at[hop],
                recv_sem=recv_two.at[hop],
                device_id={"dp": lax.rem(dp + hop, n_dp)},
                device_id_type=MESH,
            )
        )
    for copy in copies:
        copy.start()
    for copy in copies:
        copy.wait()
    planes[dp] = value
    value = planes[0]
    for plane in range(1, n_dp):
        value = value + planes[plane]
    out_ref[...] = value


def small_sums(norms, heads, n_tp, n_dp):
    width = heads.shape[1]
    return pl.pallas_call(
        functools.partial(small_sums_kernel, n_tp, n_dp),
        in_specs=[pl.BlockSpec(memory_space=pltpu.VMEM)] * 2,
        out_specs=pl.BlockSpec(memory_space=pltpu.VMEM),
        out_shape=jax.ShapeDtypeStruct((8, width), jnp.float32),
        scratch_shapes=[
            pltpu.VMEM((n_tp, 8, width), jnp.float32),
            pltpu.VMEM((8, width), jnp.float32),
            pltpu.VMEM((n_dp, 8, width), jnp.float32),
            pltpu.SemaphoreType.DMA((n_tp,)),
            pltpu.SemaphoreType.DMA((n_tp,)),
            pltpu.SemaphoreType.DMA((n_dp,)),
            pltpu.SemaphoreType.DMA((n_dp,)),
        ],
        compiler_params=pltpu.CompilerParams(collective_id=0, has_side_effects=True),
        name="small_sums",
    )(norms, heads)


def sum_groups(value, n_dp):
    if n_dp != 4:
        return lax.psum(value, "dp").astype(jnp.float32)
    place = lax.axis_index("dp")
    pair = value + lax.ppermute(value, "dp", [(0, 1), (3, 2)])
    full = pair + lax.ppermute(pair, "dp", [(1, 2), (2, 1)])
    outer = lax.ppermute(full, "dp", [(1, 0), (2, 3)])
    return jnp.where((place == 0) | (place == 3), outer, full).astype(jnp.float32)


def local(
    n_dp,
    n_tp,
    layer_input,
    segments,
    norm_gains,
    norm_biases,
    w_qkv,
    qv_bias,
    key_bias,
    w_out,
    w_gate_up,
    w_down,
    out_grad,
):
    segment_ids = segments[0]
    rows = segment_ids.shape[0]
    width = w_qkv.shape[2]
    heads = width // HEAD_DIM
    hidden = w_down.shape[0]
    cos, sin, starts = rotary_tables(segment_ids)
    start_column = jnp.broadcast_to(starts[:, None], (rows, 128))
    start_row = jnp.broadcast_to(starts[None, :], (8, rows))
    qkv_matrix = w_qkv.reshape(D, 3 * width)
    gate_matrix = w_gate_up.reshape(D, 2 * hidden)
    x_float = layer_input.astype(jnp.float32)
    normed_one, hat_one, inverse_one = norm_forward(x_float, norm_gains[0], norm_biases[0])
    rows_one = lax.all_gather(normed_one.astype(jnp.bfloat16), "tp", axis=0, tiled=True)
    portion = lax.all_gather(out_grad, "tp", axis=0, tiled=True)
    key_full = jnp.concatenate([key_bias, jnp.zeros((heads, HEAD_DIM - ROT), jnp.float32)], axis=1)
    bias_all = jnp.concatenate([qv_bias[0], key_full.reshape(width), qv_bias[1]])
    q, k, v = project(rows_one, qkv_matrix, jnp.broadcast_to(bias_all[None], (8, 3 * width)), cos, sin)
    attended, lse = attention_forward(q, k, v, start_column)
    hidden_state = x_float + lax.psum_scatter(
        jnp.dot(attended, w_out, preferred_element_type=jnp.float32).astype(jnp.bfloat16),
        "tp",
        scatter_dimension=0,
        tiled=True,
    ).astype(jnp.float32)
    normed_two, hat_two, inverse_two = norm_forward(hidden_state, norm_gains[1], norm_biases[1])
    rows_two = lax.all_gather(normed_two.astype(jnp.bfloat16), "tp", axis=0, tiled=True)
    gate_up = jnp.dot(rows_two, gate_matrix, preferred_element_type=jnp.float32)
    gate_part = gate_up[:, :hidden]
    up_part = gate_up[:, hidden:]
    sigmoid_gate = jax.nn.sigmoid(gate_part)
    silu_gate = gate_part * sigmoid_gate
    activation = (silu_gate * up_part).astype(jnp.bfloat16)
    grad_down = sum_groups(contract_rows(activation, portion).astype(jnp.bfloat16), n_dp)
    grad_act = contract_cols(portion, w_down)
    grad_gate = grad_act * up_part * sigmoid_gate * (1.0 + gate_part * (1.0 - sigmoid_gate))
    grad_up = grad_act * silu_gate
    grad_pair = jnp.concatenate([grad_gate, grad_up], axis=1).astype(jnp.bfloat16)
    grad_gate_up = jnp.concatenate(
        [
            sum_groups(contract_rows(rows_two[:, part], grad_pair).astype(jnp.bfloat16), n_dp)
            for part in (slice(0, D // 2), slice(D // 2, D))
        ]
    ).reshape(D, 2, hidden)
    grad_normed_two = lax.psum_scatter(
        contract_cols(grad_pair, gate_matrix).astype(jnp.bfloat16), "tp", scatter_dimension=0, tiled=True
    ).astype(jnp.float32)
    output = hidden_state + lax.psum_scatter(
        jnp.dot(activation, w_down, preferred_element_type=jnp.float32).astype(jnp.bfloat16),
        "tp",
        scatter_dimension=0,
        tiled=True,
    ).astype(jnp.float32)
    back_two, gain_two, shift_two = norm_backward(grad_normed_two, hat_two, inverse_two, norm_gains[1])
    grad_hidden = out_grad.astype(jnp.float32) + back_two
    branch = lax.all_gather(grad_hidden.astype(jnp.bfloat16), "tp", axis=0, tiled=True)
    grad_out = sum_groups(contract_rows(attended, branch).astype(jnp.bfloat16), n_dp)
    grad_att = contract_cols(branch, w_out).astype(jnp.bfloat16)
    grad_flat, sums = attention_backward(q, k, v, attended, grad_att, lse, start_row, cos, sin)
    grad_qkv = sum_groups(contract_rows(rows_one, grad_flat).astype(jnp.bfloat16), n_dp).reshape(D, 3, width)
    grad_normed_one = lax.psum_scatter(
        contract_cols(grad_flat, qkv_matrix).astype(jnp.bfloat16), "tp", scatter_dimension=0, tiled=True
    ).astype(jnp.float32)
    back_one, gain_one, shift_one = norm_backward(grad_normed_one, hat_one, inverse_one, norm_gains[0])
    grad_input = grad_hidden + back_one
    norms = jnp.concatenate([jnp.stack([gain_one, gain_two, shift_one, shift_two]), jnp.zeros((4, D), jnp.float32)])
    norms = norms.reshape(8, n_tp, width).transpose(1, 0, 2)
    head_sums = jnp.concatenate(
        [jnp.zeros((4, width), jnp.float32), sums[0].reshape(3, width), jnp.zeros((1, width), jnp.float32)]
    )
    small = small_sums(norms, head_sums, n_tp, n_dp)
    grad_qv = jnp.stack([small[4], small[6]])
    grad_key = small[5].reshape(heads, HEAD_DIM)[:, :ROT]
    return (output, grad_input, grad_qkv, grad_qv, grad_key, grad_out, grad_gate_up, grad_down, small[:2], small[2:4])


def solution(mesh):
    in_specs = (
        P(("dp", "tp"), None),
        P("dp", None),
        P(),
        P(),
        P(None, None, "tp"),
        P(None, "tp"),
        P("tp", None),
        P("tp", None),
        P(None, None, "tp"),
        P("tp", None),
        P(("dp", "tp"), None),
    )
    out_specs = (
        P(("dp", "tp"), None),
        P(("dp", "tp"), None),
        P(None, None, "tp"),
        P(None, "tp"),
        P("tp", None),
        P("tp", None),
        P(None, None, "tp"),
        P("tp", None),
        P(None, "tp"),
        P(None, "tp"),
    )
    body = functools.partial(local, mesh.shape["dp"], mesh.shape["tp"])
    return jax.shard_map(body, mesh=mesh, in_specs=in_specs, out_specs=out_specs, check_vma=False)
```
